32 devices in a mesh: dp: 32 (over z, y, x, core).
Axes of the slice: x: 2, y: 2, z: 4, core: 2. Of those that a mesh axis runs over, the one named last changes fastest.
Arguments:
- image_features: bfloat16 [4096, 1152], P('dp'), may hold values from -0.59765625 to 0.59765625
- text_features: bfloat16 [4096, 1152], P('dp'), may hold values from -0.59765625 to 0.59765625
- projections: bfloat16 [2304, 1152], P('dp'), may hold values from -0.1875 to 0.1875
- labels: int32 [4096], P('dp'), may hold values from 0 to 4095, as said below
Outputs:
- image_grad: float32 [4096, 1152], P('dp')
- text_grad: float32 [4096, 1152], P('dp')
The draws below stay inside these ranges and needn't reach their ends.
Inputs may be any that keep to these rules, and one draw needn't show every extreme that they name: For each block k of 128 rows, the labels are the 128 text rows of one block (k - s) mod 32, each once, with s between 0 and 15 drawn for each block.
All inputs are finite; a program needn't handle non-finite values.
Results may differ from the reference program's by a relative error of at most 0.01.
Values may be sent and summed in bfloat16 or wider, within the bound.
A program may use at most 128 MiB of HBM per device.

```python
import jax
import jax.numpy as jnp
from jax import lax

DIN = 1152
D = 1152
ROWS = 128
BLOCKS = 32
SHIFTS = 16
BATCH = 4096


def draw_labels(key, part):
    first, second = jax.random.split(jax.random.fold_in(key, 17))
    offsets = jax.random.randint(first, (BLOCKS,), 0, SHIFTS)
    keys = jax.random.split(second, BLOCKS)
    orders = jax.vmap(lambda one: jax.random.permutation(one, ROWS))(keys)
    sources = (jnp.arange(BLOCKS, dtype=jnp.int32) - offsets) % BLOCKS
    return (sources[:, None] * ROWS + orders).reshape(-1).astype(jnp.int32)


def level_of(own_key, extent, cuts, low, largest):
    gain = 1.0
    for axis_at, blocks in cuts:
        steps = jax.random.uniform(jax.random.fold_in(jax.random.fold_in(own_key, 6), axis_at), (blocks,), jnp.float32, low / len(cuts), largest / len(cuts))
        gain = gain * jnp.repeat(jnp.exp(steps), extent[axis_at] // blocks).reshape((-1,) + (1,) * (len(extent) - 1 - axis_at))
    return gain


def noise(rng, extent, deviation, reach, cuts=(), kind=jnp.bfloat16):
    result = jax.random.normal(rng, extent, jnp.float32) * deviation
    if len(cuts) > 0:
        result = level_of(rng, extent, cuts, -0.22, 0.18) * result
    return jnp.clip(result, min=-reach, max=reach).astype(kind)


def setup_inputs(seed: int = 0) -> dict:
    key_of = jax.random.split(jax.random.key(seed), 5)
    image_features = noise(key_of[0], (BATCH, DIN), 0.1, 0.59765625, ((0, 32),))
    text_features = noise(key_of[1], (BATCH, DIN), 0.1, 0.59765625, ((0, 32),))
    projections = noise(key_of[2], (2 * DIN, D), DIN ** -0.5, 0.1875, ((0, 32),))
    labels = draw_labels(jax.random.fold_in(key_of[4], 71), 0)
    return {"image_features": image_features, "text_features": text_features, "projections": projections, "labels": labels}


logit_scale = 10.0
logit_bias = -2.0
eps = 1e-06

def normalize(raw):
    norm = jnp.sqrt(lax.optimization_barrier(jnp.sum(raw * raw, axis=-1, keepdims=True)) + eps)
    return (raw / norm, norm)

def unproject(unit, norm, grad):
    inner = lax.optimization_barrier(jnp.sum(unit * grad, axis=-1, keepdims=True))
    return ((grad - unit * inner) / norm).astype(jnp.bfloat16)

def reference(image_features, text_features, projections, labels):
    width_in = image_features.shape[1]
    image_weight = projections[:width_in]
    text_weight = projections[width_in:]
    image_unit, image_norm = normalize(jnp.dot(image_features, image_weight, preferred_element_type=jnp.float32))
    text_unit, text_norm = normalize(jnp.dot(text_features, text_weight, preferred_element_type=jnp.float32))
    image_emb = image_unit.astype(jnp.bfloat16)
    text_emb = text_unit.astype(jnp.bfloat16)
    width = image_emb.shape[1]
    image_blocks = image_emb.astype(jnp.float32).reshape(BLOCKS, ROWS, width)
    text_all = text_emb.astype(jnp.float32)
    label_blocks = labels.reshape(BLOCKS, ROWS)
    positions = jnp.arange(ROWS, dtype=jnp.int32)
    owners = jnp.arange(BLOCKS, dtype=jnp.int32)

    def one_offset(offset, state):
        image_acc, text_acc = state
        offset = jnp.asarray(offset).astype(jnp.int32)
        paired = jnp.roll(text_all, offset * ROWS, axis=0).reshape(BLOCKS, ROWS, width)
        text_ids = ((owners - offset) % BLOCKS)[:, None] * ROWS + positions[None, :]
        logits = logit_scale * jnp.einsum('kid,kjd->kij', image_blocks, paired) + logit_bias
        positive = (label_blocks[:, :, None] == text_ids[:, None, :]).astype(jnp.float32)
        coeff_low = (jax.nn.sigmoid(logits) - positive).astype(jnp.bfloat16)
        coeff = lax.optimization_barrier(coeff_low).astype(jnp.float32)
        image_acc = image_acc + logit_scale * jnp.einsum('kij,kjd->kid', coeff, paired)
        text_part = logit_scale * jnp.einsum('kij,kid->kjd', coeff, image_blocks).reshape(BLOCKS * ROWS, width)
        text_acc = text_acc + jnp.roll(text_part, -offset * ROWS, axis=0)
        return (image_acc, text_acc)
    start = (jnp.zeros((BLOCKS, ROWS, width), jnp.float32), jnp.zeros((BLOCKS * ROWS, width), jnp.float32))
    image_acc, text_acc = lax.fori_loop(0, SHIFTS, one_offset, start)
    image_draw = unproject(image_unit, image_norm, image_acc.reshape(BLOCKS * ROWS, width))
    text_draw = unproject(text_unit, text_norm, text_acc)
    image_grad = jnp.dot(image_draw, image_weight.T, preferred_element_type=jnp.float32)
    text_grad = jnp.dot(text_draw, text_weight.T, preferred_element_type=jnp.float32)
    return (image_grad, text_grad)
```

```python
import functools

import jax
import jax.numpy as jnp
from jax import lax
from jax.experimental import pallas as pl
from jax.experimental.pallas import tpu as pltpu
from jax.sharding import PartitionSpec as P

REACH = 32


logit_scale = 10.0
logit_bias = -2.0
eps = 1e-06
contract_last = (((1,), (1,)), ((), ()))
MESH = pl.DeviceIdType.MESH


def normalize(raw):
    norm = jnp.sqrt(jnp.sum(raw * raw, axis=-1, keepdims=True) + eps)
    return (raw / norm, norm)


def unproject(unit, norm, grad):
    inner = jnp.sum(unit * grad, axis=-1, keepdims=True)
    return ((grad - unit * inner) / norm).astype(jnp.bfloat16)


def pair_kernel(
    count, shifts,
    image_ref, text_ref, label_ref, image_acc, text_acc,
    images, texts, names, coeff, coeff_t, over, over_in, total, total_in, back, back_in,
    send, recv,
):
    rows, width = image_ref.shape
    group = shifts // 2
    chips = group // 2
    planes = count // group
    me = lax.axis_index("dp")
    plane, inside = me // group, me % group
    chip, core = inside // 2, inside % 2
    partner = me + 1 - 2 * core

    def chip_at(step):
        return plane * group + lax.rem(chip + step + chips, chips) * 2 + core

    def plane_at(step):
        return lax.rem(plane + step + planes, planes) * group + inside

    barrier = pltpu.get_barrier_semaphore()
    others = [chip_at(step) for step in range(1, chips)]
    others += [plane_at(step) for step in (1, 2, -1, -2)] + [partner]
    for other in others:
        pl.semaphore_signal(barrier, inc=1, device_id=(other,), device_id_type=MESH)
    pl.semaphore_wait(barrier, len(others))

    made = []

    def copy(src, dst, to):
        at = len(made)
        made.append(
            pltpu.make_async_remote_copy(
                src_ref=src, dst_ref=dst, send_sem=send.at[at], recv_sem=recv.at[at],
                device_id=(to,), device_id_type=MESH,
            )
        )
        return made[-1]

    near, far = pl.ds(0, rows), pl.ds(rows, rows)
    text_copies = [copy(text_ref, texts.at[step], plane_at(step)) for step in (1, 2)]
    image_copies, name_copies = [None], [None]
    for step in range(1, chips):
        to = chip_at(step)
        name_copies.append(copy(label_ref, names.at[step, 0], to))
        image_copies.append(copy(image_ref, images.at[step, near], to))
    for one in text_copies + image_copies[1:] + name_copies[1:]:
        one.start()
    across = [
        copy(label_ref, names.at[0, 1], partner),
        copy(image_ref, images.at[0, far], partner),
    ]
    for one in across:
        one.start()
    images[0, near] = image_ref[...]
    names[0, 0] = label_ref[...]
    texts[0] = text_ref[...]
    for step in range(1, chips):
        name_copies[step].wait_recv()
        image_copies[step].wait_recv()
        passed = [
            copy(names.at[step, 0], names.at[step, 1], partner),
            copy(images.at[step, near], images.at[step, far], partner),
        ]
        for one in passed:
            one.start()
        across += passed
    for one in across:
        one.wait_recv()

    lane = lax.broadcasted_iota(jnp.int32, (rows, 1), 0)
    back_copies = []
    for age in range(3):
        if age > 0:
            text_copies[age - 1].wait_recv()
        text_block = lax.rem(me - age * group + count, count)
        ids = text_block * rows + lane
        text = texts[age]

        def fill(step, carry):
            source = lax.rem(chip - step + chips, chips)
            logits = logit_scale * lax.dot_general(
                text, images[step], contract_last, preferred_element_type=jnp.float32
            ) + logit_bias
            for side in range(2):
                block = plane * group + source * 2 + (core if side == 0 else 1 - core)
                shift = lax.rem(block - text_block + count, count)
                piece = jax.nn.sigmoid(logits[:, side * rows : (side + 1) * rows])
                piece = piece - (names[step, side] == ids).astype(jnp.float32)
                piece = piece * (shift < shifts).astype(jnp.float32)
                coeff[step, age, :, side * rows : (side + 1) * rows] = piece.astype(jnp.bfloat16)
                coeff_t[step, side * rows : (side + 1) * rows, age * rows : (age + 1) * rows] = (
                    piece.T.astype(jnp.bfloat16)
                )
            return carry

        lax.fori_loop(0, chips, fill, 0)

        def add(step, carry):
            text_acc[...] += jnp.dot(
                coeff[step, age], images[step], preferred_element_type=jnp.float32
            )
            return carry

        text_acc[...] = jnp.zeros_like(text_acc)
        lax.fori_loop(0, chips, add, 0)
        if age == 0:
            image_acc[...] = text_acc[...]
        else:
            back[age - 1] = (logit_scale * text_acc[...]).astype(jnp.bfloat16)
            back_copies.append(copy(back.at[age - 1], back_in.at[age - 1], plane_at(-age)))
            back_copies[-1].start()
    text_acc[...] = logit_scale * image_acc[...]

    rest = texts[...].reshape(3 * rows, width)

    def image_part(step, side):
        return logit_scale * jnp.dot(
            coeff_t[step, side * rows : (side + 1) * rows], rest,
            preferred_element_type=jnp.float32,
        )

    over_copies = []
    steps = list(range(1, chips)) + [0]
    for step in steps:
        over[step] = image_part(step, 1).astype(jnp.bfloat16)
        over_copies.append(copy(over.at[step], over_in.at[step], partner))
        over_copies[-1].start()
    total_copies = []
    for at, step in enumerate(steps):
        mine = image_part(step, 0)
        over_copies[at].wait_recv()
        mine = mine + over_in[step].astype(jnp.float32)
        if step == 0:
            image_acc[...] = mine
        else:
            total[step] = mine.astype(jnp.bfloat16)
            total_copies.append(copy(total.at[step], total_in.at[step], chip_at(-step)))
            total_copies[-1].start()
    for at in range(chips - 1):
        total_copies[at].wait_recv()
        image_acc[...] += total_in[at + 1].astype(jnp.float32)
    for age in range(2):
        back_copies[age].wait_recv()
        text_acc[...] += back_in[age].astype(jnp.float32)
    for one in made:
        one.wait_send()


def pair_grads(image_emb, text_emb, labels, count, shifts):
    rows, width = image_emb.shape
    chips = shifts // 4
    low = jnp.bfloat16
    copies = 2 + 6 * chips + 2
    vmem = pl.BlockSpec(memory_space=pltpu.VMEM)
    return pl.pallas_call(
        functools.partial(pair_kernel, count, shifts),
        out_shape=[jax.ShapeDtypeStruct((rows, width), jnp.float32)] * 2,
        in_specs=[vmem] * 3,
        out_specs=[vmem] * 2,
        scratch_shapes=[
            pltpu.VMEM((chips, 2 * rows, width), low),
            pltpu.VMEM((3, rows, width), low),
            pltpu.VMEM((chips, 2, 1, rows), jnp.int32),
            pltpu.VMEM((chips, 3, rows, 2 * rows), low),
            pltpu.VMEM((chips, 2 * rows, 3 * rows), low),
            pltpu.VMEM((chips, rows, width), low),
            pltpu.VMEM((chips, rows, width), low),
            pltpu.VMEM((chips, rows, width), low),
            pltpu.VMEM((chips, rows, width), low),
            pltpu.VMEM((2, rows, width), low),
            pltpu.VMEM((2, rows, width), low),
            pltpu.SemaphoreType.DMA((copies,)),
            pltpu.SemaphoreType.DMA((copies,)),
        ],
        compiler_params=pltpu.CompilerParams(
            collective_id=0, has_side_effects=True, vmem_limit_bytes=60 * 1024 * 1024
        ),
    )(image_emb, text_emb, labels.reshape(1, rows))


def per_device(image_features, text_features, projections, labels):
    rows, width_in = image_features.shape
    count = lax.axis_size("dp")
    shifts = min(REACH, count // 2)
    whole = lax.all_gather(projections, "dp", axis=0, tiled=True)
    image_weight = whole[:width_in]
    text_weight = whole[width_in:]
    image_unit, image_norm = normalize(
        jnp.dot(image_features, image_weight, preferred_element_type=jnp.float32)
    )
    text_unit, text_norm = normalize(
        jnp.dot(text_features, text_weight, preferred_element_type=jnp.float32)
    )
    image_acc, text_acc = pair_grads(
        image_unit.astype(jnp.bfloat16), text_unit.astype(jnp.bfloat16), labels, count, shifts
    )
    image_draw = unproject(image_unit, image_norm, image_acc)
    text_draw = unproject(text_unit, text_norm, text_acc)
    image_grad = lax.dot_general(
        image_draw, image_weight, contract_last, preferred_element_type=jnp.float32
    )
    text_grad = lax.dot_general(
        text_draw, text_weight, contract_last, preferred_element_type=jnp.float32
    )
    return (image_grad, text_grad)


def solution(mesh):
    placed = (P("dp", None), P("dp", None), P("dp", None), P("dp"))
    return jax.shard_map(
        per_device,
        mesh=mesh,
        in_specs=placed,
        out_specs=(P("dp", None), P("dp", None)),
        check_vma=False,
    )
```

```python
import functools

import jax
import jax.numpy as jnp
from jax import lax
from jax.experimental import pallas as pl
from jax.experimental.pallas import tpu as pltpu
from jax.sharding import PartitionSpec as P

REACH = 32


logit_scale = 10.0
logit_bias = -2.0
eps = 1e-06
contract_last = (((1,), (1,)), ((), ()))
MESH = pl.DeviceIdType.MESH


def normalize(raw):
    norm = jnp.sqrt(jnp.sum(raw * raw, axis=-1, keepdims=True) + eps)
    return (raw / norm, norm)


def unproject(unit, norm, grad):
    inner = jnp.sum(unit * grad, axis=-1, keepdims=True)
    return ((grad - unit * inner) / norm).astype(jnp.bfloat16)


def pair_kernel(
    count, shifts,
    image_ref, text_ref, label_ref, image_acc, text_acc,
    images, texts, names, coeff, coeff_t, over, over_in, total, total_in, back, back_in,
    send, recv,
):
    rows, width = image_ref.shape
    group = shifts // 2
    chips = group // 2
    planes = count // group
    me = lax.axis_index("dp")
    plane, inside = me // group, me % group
    chip, core = inside // 2, inside % 2
    partner = me + 1 - 2 * core

    def chip_at(step):
        return plane * group + lax.rem(chip + step + chips, chips) * 2 + core

    def plane_at(step):
        return lax.rem(plane + step + planes, planes) * group + inside

    barrier = pltpu.get_barrier_semaphore()
    others = [chip_at(step) for step in range(1, chips)]
    others += [plane_at(step) for step in (1, 2, -1, -2)] + [partner]
    for other in others:
        pl.semaphore_signal(barrier, inc=1, device_id=(other,), device_id_type=MESH)
    pl.semaphore_wait(barrier, len(others))

    made = []

    def copy(src, dst, to):
        at = len(made)
        made.append(
            pltpu.make_async_remote_copy(
                src_ref=src, dst_ref=dst, send_sem=send.at[at], recv_sem=recv.at[at],
                device_id=(to,), device_id_type=MESH,
            )
        )
        return made[-1]

    near, far = pl.ds(0, rows), pl.ds(rows, rows)
    text_copies = [copy(text_ref, texts.at[step], plane_at(step)) for step in (1, 2)]
    image_copies, name_copies = [None], [None]
    for step in range(1, chips):
        to = chip_at(step)
        name_copies.append(copy(label_ref, names.at[step, 0], to))
        image_copies.append(copy(image_ref, images.at[step, near], to))
    for one in text_copies + image_copies[1:] + name_copies[1:]:
        one.start()
    across = [
        copy(label_ref, names.at[0, 1], partner),
        copy(image_ref, images.at[0, far], partner),
    ]
    for one in across:
        one.start()
    images[0, near] = image_ref[...]
    names[0, 0] = label_ref[...]
    texts[0] = text_ref[...]
    for step in range(1, chips):
        name_copies[step].wait_recv()
        image_copies[step].wait_recv()
        passed = [
            copy(names.at[step, 0], names.at[step, 1], partner),
            copy(images.at[step, near], images.at[step, far], partner),
        ]
        for one in passed:
            one.start()
        across += passed
    for one in across:
        one.wait_recv()

    lane = lax.broadcasted_iota(jnp.int32, (rows, 1), 0)
    back_copies = []
    for age in range(3):
        if age > 0:
            text_copies[age - 1].wait_recv()
        text_block = lax.rem(me - age * group + count, count)
        ids = text_block * rows + lane
        text = texts[age]

        def fill(step, carry):
            source = lax.rem(chip - step + chips, chips)
            logits = logit_scale * lax.dot_general(
                text, images[step], contract_last, preferred_element_type=jnp.float32
            ) + logit_bias
            for side in range(2):
                block = plane * group + source * 2 + (core if side == 0 else 1 - core)
                shift = lax.rem(block - text_block + count, count)
                piece = jax.nn.sigmoid(logits[:, side * rows : (side + 1) * rows])
                piece = piece - (names[step, side] == ids).astype(jnp.float32)
                piece = piece * (shift < shifts).astype(jnp.float32)
                coeff[step, age, :, side * rows : (side + 1) * rows] = piece.astype(jnp.bfloat16)
                coeff_t[step, side * rows : (side + 1) * rows, age * rows : (age + 1) * rows] = (
                    piece.T.astype(jnp.bfloat16)
                )
            return carry

        lax.fori_loop(0, chips, fill, 0)

        def add(step, carry):
            text_acc[...] += jnp.dot(
                coeff[step, age], images[step], preferred_element_type=jnp.float32
            )
            return carry

        text_acc[...] = jnp.zeros_like(text_acc)
        lax.fori_loop(0, chips, add, 0)
        if age == 0:
            image_acc[...] = text_acc[...]
        else:
            back[age - 1] = (logit_scale * text_acc[...]).astype(jnp.bfloat16)
            back_copies.append(copy(back.at[age - 1], back_in.at[age - 1], plane_at(-age)))
            back_copies[-1].start()
    text_acc[...] = logit_scale * image_acc[...]

    rest = texts[...].reshape(3 * rows, width)

    def image_part(step, side):
        return logit_scale * jnp.dot(
            coeff_t[step, side * rows : (side + 1) * rows], rest,
            preferred_element_type=jnp.float32,
        )

    over_copies = []
    steps = list(range(1, chips)) + [0]
    for step in steps:
        over[step] = image_part(step, 1).astype(jnp.bfloat16)
        over_copies.append(copy(over.at[step], over_in.at[step], partner))
        over_copies[-1].start()
    total_copies = []
    for at, step in enumerate(steps):
        mine = image_part(step, 0)
        over_copies[at].wait_recv()
        mine = mine + over_in[step].astype(jnp.float32)
        if step == 0:
            image_acc[...] = mine
        else:
            total[step] = mine.astype(jnp.bfloat16)
            total_copies.append(copy(total.at[step], total_in.at[step], chip_at(-step)))
            total_copies[-1].start()
    for at in range(chips - 1):
        total_copies[at].wait_recv()
        image_acc[...] += total_in[at + 1].astype(jnp.float32)
    for age in range(2):
        back_copies[age].wait_recv()
        text_acc[...] += back_in[age].astype(jnp.float32)
    for one in made:
        one.wait_send()


def pair_grads(image_emb, text_emb, labels, count, shifts):
    rows, width = image_emb.shape
    chips = shifts // 4
    low = jnp.bfloat16
    copies = 2 + 6 * chips + 2
    vmem = pl.BlockSpec(memory_space=pltpu.VMEM)
    return pl.pallas_call(
        functools.partial(pair_kernel, count, shifts),
        out_shape=[jax.ShapeDtypeStruct((rows, width), jnp.float32)] * 2,
        in_specs=[vmem] * 3,
        out_specs=[vmem] * 2,
        scratch_shapes=[
            pltpu.VMEM((chips, 2 * rows, width), low),
            pltpu.VMEM((3, rows, width), low),
            pltpu.VMEM((chips, 2, 1, rows), jnp.int32),
            pltpu.VMEM((chips, 3, rows, 2 * rows), low),
            pltpu.VMEM((chips, 2 * rows, 3 * rows), low),
            pltpu.VMEM((chips, rows, width), low),
            pltpu.VMEM((chips, rows, width), low),
            pltpu.VMEM((chips, rows, width), low),
            pltpu.VMEM((chips, rows, width), low),
            pltpu.VMEM((2, rows, width), low),
            pltpu.VMEM((2, rows, width), low),
            pltpu.SemaphoreType.DMA((copies,)),
            pltpu.SemaphoreType.DMA((copies,)),
        ],
        compiler_params=pltpu.CompilerParams(
            collective_id=0, has_side_effects=True, vmem_limit_bytes=60 * 1024 * 1024
        ),
    )(image_emb, text_emb, labels.reshape(1, rows))


def gather_kernel(count, group, shard_ref, whole_ref, send, recv):
    chips, planes = group // 2, count // group
    me = lax.axis_index("dp")
    plane, inside = me // group, me % group
    chip, core = inside // 2, inside % 2
    partner = me + 1 - 2 * core
    relayed = chips == 4
    if relayed:
        low, high = chip + 1 - 2 * lax.rem(chip, 2), lax.rem(chip + 2, 4)
        peers = [low + (high - low) * core, high + (low - high) * core]
        sources = peers
    else:
        peers = [lax.rem(chip + step, chips) for step in range(1, chips)]
        sources = [lax.rem(chip + chips - step, chips) for step in range(1, chips)]

    def plane_at(step):
        return lax.rem(plane + step + planes, planes)

    def device(plane, chip):
        return plane * group + chip * 2 + core

    barrier = pltpu.get_barrier_semaphore()
    others = [device(plane, peer) for peer in peers]
    others += [device(plane_at(step), chip) for step in range(1, planes)] + [partner]
    for other in others:
        pl.semaphore_signal(barrier, inc=1, device_id=(other,), device_id_type=MESH)
    pl.semaphore_wait(barrier, len(others))

    made = []

    def copy(slot, to, src=None):
        at = len(made)
        made.append(
            pltpu.make_async_remote_copy(
                src_ref=whole_ref.at[slot] if src is None else src,
                dst_ref=whole_ref.at[slot],
                send_sem=send.at[at], recv_sem=recv.at[at],
                device_id=(to,), device_id_type=MESH,
            )
        )
        made[-1].start()
        return made[-1]

    between = [copy(me, device(plane_at(step), chip), shard_ref) for step in range(1, planes)]
    within, final = [], []
    for step in range(planes + 1):
        if step < planes:
            held = plane_at(-step)
            slot = device(held, chip)
            if step > 0:
                between[step - 1].wait_recv()
            src = shard_ref if step == 0 else None
            within.append([copy(slot, device(plane, peer), src) for peer in peers])
            final.append(copy(slot, partner, src))
            if step == 0:
                whole_ref[me] = shard_ref[...]
        if step > 0:
            held = plane_at(1 - step)
            for at, source in enumerate(sources):
                within[step - 1][at].wait_recv()
                slot = device(held, source)
                if relayed and at == 0:
                    relay = copy(slot, device(plane, peers[1]))
                final.append(copy(slot, partner))
            if relayed:
                relay.wait_recv()
                final.append(copy(device(held, 3 - chip), partner))
    for one in final:
        one.wait_recv()
    for one in made:
        one.wait_send()


def gather(shard, count, group):
    planes, chips = count // group, group // 2
    copies = planes - 1 + planes * (2 * chips - 1)
    vmem = pl.BlockSpec(memory_space=pltpu.VMEM)
    return pl.pallas_call(
        functools.partial(gather_kernel, count, group),
        out_shape=jax.ShapeDtypeStruct((count,) + shard.shape, shard.dtype),
        in_specs=[vmem],
        out_specs=vmem,
        scratch_shapes=[pltpu.SemaphoreType.DMA((copies,)), pltpu.SemaphoreType.DMA((copies,))],
        compiler_params=pltpu.CompilerParams(
            collective_id=1, has_side_effects=True, vmem_limit_bytes=40 * 1024 * 1024
        ),
    )(shard)


def per_device(image_features, text_features, projections, labels):
    rows, width_in = image_features.shape
    count = lax.axis_size("dp")
    shifts = min(REACH, count // 2)
    whole = gather(projections, count, shifts // 2).reshape(2 * width_in, -1)
    image_weight = whole[:width_in]
    text_weight = whole[width_in:]
    image_unit, image_norm = normalize(
        jnp.dot(image_features, image_weight, preferred_element_type=jnp.float32)
    )
    text_unit, text_norm = normalize(
        jnp.dot(text_features, text_weight, preferred_element_type=jnp.float32)
    )
    image_acc, text_acc = pair_grads(
        image_unit.astype(jnp.bfloat16), text_unit.astype(jnp.bfloat16), labels, count, shifts
    )
    image_draw = unproject(image_unit, image_norm, image_acc)
    text_draw = unproject(text_unit, text_norm, text_acc)
    image_grad = lax.dot_general(
        image_draw, image_weight, contract_last, preferred_element_type=jnp.float32
    )
    text_grad = lax.dot_general(
        text_draw, text_weight, contract_last, preferred_element_type=jnp.float32
    )
    return (image_grad, text_grad)


def solution(mesh):
    placed = (P("dp", None), P("dp", None), P("dp", None), P("dp"))
    return jax.shard_map(
        per_device,
        mesh=mesh,
        in_specs=placed,
        out_specs=(P("dp", None), P("dp", None)),
        check_vma=False,
    )
```

```python
import functools

import jax
import jax.numpy as jnp
from jax import lax
from jax.experimental import pallas as pl
from jax.experimental.pallas import tpu as pltpu
from jax.sharding import PartitionSpec as P

REACH = 32


logit_scale = 10.0
logit_bias = -2.0
eps = 1e-06
contract_last = (((1,), (1,)), ((), ()))
MESH = pl.DeviceIdType.MESH


def normalize(raw):
    norm = jnp.sqrt(jnp.sum(raw * raw, axis=-1, keepdims=True) + eps)
    return (raw / norm, norm)


def unproject(unit, norm, grad):
    inner = jnp.sum(unit * grad, axis=-1, keepdims=True)
    return ((grad - unit * inner) / norm).astype(jnp.bfloat16)


def pair_kernel(
    count, shifts,
    image_ref, texts, label_ref, image_acc, text_acc,
    images, names, coeff, coeff_t, text_sum, over, over_in, total, total_in, back, back_in,
    send, recv,
):
    rows, width = image_ref.shape
    group = shifts // 2
    chips = group // 2
    planes = count // group
    me = lax.axis_index("dp")
    plane, inside = me // group, me % group
    chip, core = inside // 2, inside % 2
    partner = me + 1 - 2 * core

    def chip_at(step):
        return plane * group + lax.rem(chip + step + chips, chips) * 2 + core

    def plane_at(step):
        return lax.rem(plane + step + planes, planes) * group + inside

    barrier = pltpu.get_barrier_semaphore()
    others = [chip_at(step) for step in range(1, chips)]
    others += [plane_at(step) for step in (1, 2, -1, -2)] + [partner]
    for other in others:
        pl.semaphore_signal(barrier, inc=1, device_id=(other,), device_id_type=MESH)
    pl.semaphore_wait(barrier, len(others))

    made = []

    def copy(src, dst, to):
        at = len(made)
        made.append(
            pltpu.make_async_remote_copy(
                src_ref=src, dst_ref=dst, send_sem=send.at[at], recv_sem=recv.at[at],
                device_id=(to,), device_id_type=MESH,
            )
        )
        made[-1].start()
        return made[-1]

    near, far = pl.ds(0, rows), pl.ds(rows, rows)
    across = [
        [
            copy(label_ref, names.at[0, 1], partner),
            copy(image_ref, images.at[0, far], partner),
        ]
    ]
    arrivals = [[]]
    for step in range(1, chips):
        to = chip_at(step)
        arrivals.append(
            [
                copy(label_ref, names.at[step, 0], to),
                copy(image_ref, images.at[step, near], to),
            ]
        )
    images[0, near] = image_ref[...]
    names[0, 0] = label_ref[...]
    lane = lax.broadcasted_iota(jnp.int32, (rows, 1), 0)

    def pass_on(step):
        for one in arrivals[step]:
            one.wait_recv()
        across.append(
            [
                copy(names.at[step, 0], names.at[step, 1], partner),
                copy(images.at[step, near], images.at[step, far], partner),
            ]
        )

    def fill(step):
        source = lax.rem(chip - step + chips, chips)
        logits = logit_scale * lax.dot_general(
            texts[...], images[step], contract_last, preferred_element_type=jnp.float32
        ) + logit_bias
        for age in range(3):
            text_block = lax.rem(me - age * group + count, count)
            ids = text_block * rows + lane
            lines = slice(age * rows, (age + 1) * rows)
            for side in range(2):
                block = plane * group + source * 2 + (core if side == 0 else 1 - core)
                shift = lax.rem(block - text_block + count, count)
                span = slice(side * rows, (side + 1) * rows)
                piece = jax.nn.sigmoid(logits[lines, span])
                piece = piece - (names[step, side] == ids).astype(jnp.float32)
                piece = piece * (shift < shifts).astype(jnp.float32)
                coeff[lines, span] = piece.astype(jnp.bfloat16)
                coeff_t[span, lines] = piece.T.astype(jnp.bfloat16)

    def image_part(side):
        return logit_scale * jnp.dot(
            coeff_t[side * rows : (side + 1) * rows], texts[...],
            preferred_element_type=jnp.float32,
        )

    def text_part(step, age):
        lines = slice(age * rows, (age + 1) * rows)
        part = jnp.dot(coeff[lines], images[step], preferred_element_type=jnp.float32)
        return part if step == 0 else text_sum[lines] + part

    over_copies, total_copies, back_copies = [], [], {}

    def settle(step):
        over_copies[step].wait_recv()
        if step == 0:
            image_acc[...] = image_acc[...] + over_in[0].astype(jnp.float32)
        else:
            total[step] = (kept[step] + over_in[step].astype(jnp.float32)).astype(jnp.bfloat16)
            total_copies.append(copy(total.at[step], total_in.at[step], chip_at(-step)))

    kept = {}
    for step in range(chips):
        for one in across[step]:
            one.wait_recv()
        fill(step)
        if step + 1 < chips:
            pass_on(step + 1)
            for age in range(3):
                text_sum[age * rows : (age + 1) * rows] = text_part(step, age)
        else:
            for age in (2, 1):
                back[age - 1] = (logit_scale * text_part(step, age)).astype(jnp.bfloat16)
                back_copies[age] = copy(back.at[age - 1], back_in.at[age - 1], plane_at(-age))
        over[step] = image_part(1).astype(jnp.bfloat16)
        over_copies.append(copy(over.at[step], over_in.at[step], partner))
        if step == 0:
            image_acc[...] = image_part(0)
        else:
            kept[step] = image_part(0)
        if step > 0:
            settle(step - 1)
        if step + 1 == chips:
            text_acc[...] = logit_scale * text_part(step, 0)
            settle(step)
    for at in range(chips - 1):
        total_copies[at].wait_recv()
        image_acc[...] += total_in[at + 1].astype(jnp.float32)
    for age in (1, 2):
        back_copies[age].wait_recv()
        text_acc[...] += back_in[age - 1].astype(jnp.float32)
    for one in made:
        one.wait_send()


def pair_grads(image_emb, text_embs, labels, count, shifts):
    rows, width = image_emb.shape
    chips = shifts // 4
    low = jnp.bfloat16
    copies = 6 * chips + 2
    vmem = pl.BlockSpec(memory_space=pltpu.VMEM)
    return pl.pallas_call(
        functools.partial(pair_kernel, count, shifts),
        out_shape=[jax.ShapeDtypeStruct((rows, width), jnp.float32)] * 2,
        in_specs=[vmem] * 3,
        out_specs=[vmem] * 2,
        scratch_shapes=[
            pltpu.VMEM((chips, 2 * rows, width), low),
            pltpu.VMEM((chips, 2, 1, rows), jnp.int32),
            pltpu.VMEM((3 * rows, 2 * rows), low),
            pltpu.VMEM((2 * rows, 3 * rows), low),
            pltpu.VMEM((3 * rows, width), jnp.float32),
            pltpu.VMEM((chips, rows, width), low),
            pltpu.VMEM((chips, rows, width), low),
            pltpu.VMEM((chips, rows, width), low),
            pltpu.VMEM((chips, rows, width), low),
            pltpu.VMEM((2, rows, width), low),
            pltpu.VMEM((2, rows, width), low),
            pltpu.SemaphoreType.DMA((copies,)),
            pltpu.SemaphoreType.DMA((copies,)),
        ],
        compiler_params=pltpu.CompilerParams(
            collective_id=0, has_side_effects=True, vmem_limit_bytes=48 * 1024 * 1024
        ),
    )(image_emb, text_embs, labels.reshape(1, rows))


def gather_kernel(count, group, shard_ref, text_ref, whole_ref, texts_ref, send, recv):
    chips, planes = group // 2, count // group
    me = lax.axis_index("dp")
    plane, inside = me // group, me % group
    chip, core = inside // 2, inside % 2
    partner = me + 1 - 2 * core
    relayed = chips == 4
    if relayed:
        low, high = chip + 1 - 2 * lax.rem(chip, 2), lax.rem(chip + 2, 4)
        peers = [low + (high - low) * core, high + (low - high) * core]
        sources = peers
    else:
        peers = [lax.rem(chip + step, chips) for step in range(1, chips)]
        sources = [lax.rem(chip + chips - step, chips) for step in range(1, chips)]

    def plane_at(step):
        return lax.rem(plane + step + planes, planes)

    def device(plane, chip):
        return plane * group + chip * 2 + core

    barrier = pltpu.get_barrier_semaphore()
    others = [device(plane, peer) for peer in peers]
    others += [device(plane_at(step), chip) for step in range(1, planes)] + [partner]
    for other in others:
        pl.semaphore_signal(barrier, inc=1, device_id=(other,), device_id_type=MESH)
    pl.semaphore_wait(barrier, len(others))

    made = []

    def copy(slot, to, src=None, dst=None):
        at = len(made)
        made.append(
            pltpu.make_async_remote_copy(
                src_ref=whole_ref.at[slot] if src is None else src,
                dst_ref=whole_ref.at[slot] if dst is None else dst,
                send_sem=send.at[at], recv_sem=recv.at[at],
                device_id=(to,), device_id_type=MESH,
            )
        )
        made[-1].start()
        return made[-1]

    between = [copy(me, device(plane_at(step), chip), shard_ref) for step in range(1, planes)]
    within, final = [], []
    for step in range(planes + 1):
        if step < planes:
            held = plane_at(-step)
            slot = device(held, chip)
            if step > 0:
                between[step - 1].wait_recv()
            src = shard_ref if step == 0 else None
            within.append([copy(slot, device(plane, peer), src) for peer in peers])
            final.append(copy(slot, partner, src))
            if step == 0:
                whole_ref[me] = shard_ref[...]
                texts_ref[0] = text_ref[...]
            if step == planes - 1:
                for age in (2, 1):
                    to = device(plane_at(age), chip)
                    final.append(copy(None, to, text_ref, texts_ref.at[age]))
        if step > 0:
            held = plane_at(1 - step)
            for at, source in enumerate(sources):
                within[step - 1][at].wait_recv()
                slot = device(held, source)
                if relayed and at == 0:
                    relay = copy(slot, device(plane, peers[1]))
                final.append(copy(slot, partner))
            if relayed:
                relay.wait_recv()
                final.append(copy(device(held, 3 - chip), partner))
    for one in final:
        one.wait_recv()
    for one in made:
        one.wait_send()


def gather(shard, text, count, group):
    planes, chips = count // group, group // 2
    copies = planes + 1 + planes * (2 * chips - 1)
    vmem = pl.BlockSpec(memory_space=pltpu.VMEM)
    return pl.pallas_call(
        functools.partial(gather_kernel, count, group),
        out_shape=[
            jax.ShapeDtypeStruct((count,) + shard.shape, shard.dtype),
            jax.ShapeDtypeStruct((3,) + text.shape, text.dtype),
        ],
        in_specs=[vmem] * 2,
        out_specs=[vmem] * 2,
        scratch_shapes=[pltpu.SemaphoreType.DMA((copies,)), pltpu.SemaphoreType.DMA((copies,))],
        compiler_params=pltpu.CompilerParams(
            collective_id=1, has_side_effects=True, vmem_limit_bytes=40 * 1024 * 1024
        ),
    )(shard, text)


def per_device(image_features, text_features, projections, labels):
    rows, width_in = image_features.shape
    count = lax.axis_size("dp")
    shifts = min(REACH, count // 2)
    whole, texts = gather(projections, text_features, count, shifts // 2)
    whole = whole.reshape(2 * width_in, -1)
    image_weight = whole[:width_in]
    text_weight = whole[width_in:]
    image_unit, image_norm = normalize(
        jnp.dot(image_features, image_weight, preferred_element_type=jnp.float32)
    )
    text_units, text_norms = normalize(
        jnp.dot(
            texts.reshape(3 * rows, width_in), text_weight, preferred_element_type=jnp.float32
        )
    )
    text_unit, text_norm = text_units[:rows], text_norms[:rows]
    image_acc, text_acc = pair_grads(
        image_unit.astype(jnp.bfloat16), text_units.astype(jnp.bfloat16), labels, count, shifts
    )
    image_draw = unproject(image_unit, image_norm, image_acc)
    text_draw = unproject(text_unit, text_norm, text_acc)
    image_grad = lax.dot_general(
        image_draw, image_weight, contract_last, preferred_element_type=jnp.float32
    )
    text_grad = lax.dot_general(
        text_draw, text_weight, contract_last, preferred_element_type=jnp.float32
    )
    return (image_grad, text_grad)


def solution(mesh):
    placed = (P("dp", None), P("dp", None), P("dp", None), P("dp"))
    return jax.shard_map(
        per_device,
        mesh=mesh,
        in_specs=placed,
        out_specs=(P("dp", None), P("dp", None)),
        check_vma=False,
    )
```

```python
import functools

import jax
import jax.numpy as jnp
from jax import lax
from jax.experimental import pallas as pl
from jax.experimental.pallas import tpu as pltpu
from jax.sharding import PartitionSpec as P

REACH = 32


logit_scale = 10.0
logit_bias = -2.0
eps = 1e-06
contract_last = (((1,), (1,)), ((), ()))
MESH = pl.DeviceIdType.MESH


def normalize(raw):
    norm = jnp.sqrt(jnp.sum(raw * raw, axis=-1, keepdims=True) + eps)
    return (raw / norm, norm)


def unproject(unit, norm, grad):
    inner = jnp.sum(unit * grad, axis=-1, keepdims=True)
    return ((grad - unit * inner) / norm).astype(jnp.bfloat16)


def pair_kernel(
    count, shifts,
    image_ref, texts, label_ref, image_acc, text_acc,
    images, names, coeff, coeff_t, text_sum, over, over_in, total, total_in, back, back_in,
    send, recv,
):
    rows, width = image_ref.shape
    group = shifts // 2
    chips = group // 2
    planes = count // group
    me = lax.axis_index("dp")
    plane, inside = me // group, me % group
    chip, core = inside // 2, inside % 2
    partner = me + 1 - 2 * core

    def chip_at(step):
        return plane * group + lax.rem(chip + step + chips, chips) * 2 + core

    def plane_at(step):
        return lax.rem(plane + step + planes, planes) * group + inside

    barrier = pltpu.get_barrier_semaphore()
    others = [chip_at(step) for step in range(1, chips)]
    others += [plane_at(step) for step in (1, 2, -1, -2)] + [partner]
    for other in others:
        pl.semaphore_signal(barrier, inc=1, device_id=(other,), device_id_type=MESH)
    pl.semaphore_wait(barrier, len(others))

    made = []

    def copy(src, dst, to):
        at = len(made)
        made.append(
            pltpu.make_async_remote_copy(
                src_ref=src, dst_ref=dst, send_sem=send.at[at], recv_sem=recv.at[at],
                device_id=(to,), device_id_type=MESH,
            )
        )
        made[-1].start()
        return made[-1]

    near, far = pl.ds(0, rows), pl.ds(rows, rows)
    across = [
        [
            copy(label_ref, names.at[0, 1], partner),
            copy(image_ref, images.at[0, far], partner),
        ]
    ]
    arrivals = [[]]
    for step in range(1, chips):
        to = chip_at(step)
        arrivals.append(
            [
                copy(label_ref, names.at[step, 0], to),
                copy(image_ref, images.at[step, near], to),
            ]
        )
    images[0, near] = image_ref[...]
    names[0, 0] = label_ref[...]
    lane = lax.broadcasted_iota(jnp.int32, (rows, 1), 0)

    def pass_on(step):
        for one in arrivals[step]:
            one.wait_recv()
        across.append(
            [
                copy(names.at[step, 0], names.at[step, 1], partner),
                copy(images.at[step, near], images.at[step, far], partner),
            ]
        )

    def fill(step):
        source = lax.rem(chip - step + chips, chips)
        logits = logit_scale * lax.dot_general(
            texts[...], images[step], contract_last, preferred_element_type=jnp.float32
        ) + logit_bias
        for age in range(3):
            text_block = lax.rem(me - age * group + count, count)
            ids = text_block * rows + lane
            lines = slice(age * rows, (age + 1) * rows)
            for side in range(2):
                block = plane * group + source * 2 + (core if side == 0 else 1 - core)
                shift = lax.rem(block - text_block + count, count)
                span = slice(side * rows, (side + 1) * rows)
                piece = jax.nn.sigmoid(logits[lines, span])
                piece = piece - (names[step, side] == ids).astype(jnp.float32)
                piece = piece * (shift < shifts).astype(jnp.float32)
                coeff[lines, span] = piece.astype(jnp.bfloat16)
                coeff_t[span, lines] = piece.T.astype(jnp.bfloat16)

    def image_part(side):
        return logit_scale * jnp.dot(
            coeff_t[side * rows : (side + 1) * rows], texts[...],
            preferred_element_type=jnp.float32,
        )

    def text_part(step, age):
        lines = slice(age * rows, (age + 1) * rows)
        part = jnp.dot(coeff[lines], images[step], preferred_element_type=jnp.float32)
        return part if step == 0 else text_sum[lines] + part

    over_copies, total_copies, back_copies = [], [], {}

    def settle(step):
        over_copies[step].wait_recv()
        if step == 0:
            image_acc[...] = image_acc[...] + over_in[0].astype(jnp.float32)
        else:
            total[step] = (kept[step] + over_in[step].astype(jnp.float32)).astype(jnp.bfloat16)
            total_copies.append(copy(total.at[step], total_in.at[step], chip_at(-step)))

    kept = {}
    for step in range(chips):
        for one in across[step]:
            one.wait_recv()
        fill(step)
        if step + 1 < chips:
            pass_on(step + 1)
            for age in range(3):
                text_sum[age * rows : (age + 1) * rows] = text_part(step, age)
        else:
            for age in (2, 1):
                back[age - 1] = (logit_scale * text_part(step, age)).astype(jnp.bfloat16)
                back_copies[age] = copy(back.at[age - 1], back_in.at[age - 1], plane_at(-age))
        over[step] = image_part(1).astype(jnp.bfloat16)
        over_copies.append(copy(over.at[step], over_in.at[step], partner))
        if step == 0:
            image_acc[...] = image_part(0)
        else:
            kept[step] = image_part(0)
        if step > 0:
            settle(step - 1)
        if step + 1 == chips:
            text_acc[...] = logit_scale * text_part(step, 0)
            settle(step)
    for at in range(chips - 1):
        total_copies[at].wait_recv()
        image_acc[...] += total_in[at + 1].astype(jnp.float32)
    for age in (1, 2):
        back_copies[age].wait_recv()
        text_acc[...] += back_in[age - 1].astype(jnp.float32)
    for one in made:
        one.wait_send()


def pair_grads(image_emb, text_embs, labels, count, shifts):
    rows, width = image_emb.shape
    chips = shifts // 4
    low = jnp.bfloat16
    copies = 6 * chips + 2
    vmem = pl.BlockSpec(memory_space=pltpu.VMEM)
    return pl.pallas_call(
        functools.partial(pair_kernel, count, shifts),
        out_shape=[jax.ShapeDtypeStruct((rows, width), jnp.float32)] * 2,
        in_specs=[vmem] * 3,
        out_specs=[vmem] * 2,
        scratch_shapes=[
            pltpu.VMEM((chips, 2 * rows, width), low),
            pltpu.VMEM((chips, 2, 1, rows), jnp.int32),
            pltpu.VMEM((3 * rows, 2 * rows), low),
            pltpu.VMEM((2 * rows, 3 * rows), low),
            pltpu.VMEM((3 * rows, width), jnp.float32),
            pltpu.VMEM((chips, rows, width), low),
            pltpu.VMEM((chips, rows, width), low),
            pltpu.VMEM((chips, rows, width), low),
            pltpu.VMEM((chips, rows, width), low),
            pltpu.VMEM((2, rows, width), low),
            pltpu.VMEM((2, rows, width), low),
            pltpu.SemaphoreType.DMA((copies,)),
            pltpu.SemaphoreType.DMA((copies,)),
        ],
        compiler_params=pltpu.CompilerParams(
            collective_id=0, has_side_effects=True, vmem_limit_bytes=48 * 1024 * 1024
        ),
    )(image_emb, text_embs, labels.reshape(1, rows))


def gather_kernel(count, group, shard_ref, text_ref, whole_ref, texts_ref, send, recv):
    chips, planes = group // 2, count // group
    me = lax.axis_index("dp")
    plane, inside = me // group, me % group
    chip, core = inside // 2, inside % 2
    partner = me + 1 - 2 * core
    relayed = chips == 4
    if relayed:
        low, high = chip + 1 - 2 * lax.rem(chip, 2), lax.rem(chip + 2, 4)
        peers = [low + (high - low) * core, high + (low - high) * core]
        sources = peers
    else:
        peers = [lax.rem(chip + step, chips) for step in range(1, chips)]
        sources = [lax.rem(chip + chips - step, chips) for step in range(1, chips)]

    def plane_at(step):
        return lax.rem(plane + step + planes, planes)

    def device(plane, chip):
        return plane * group + chip * 2 + core

    barrier = pltpu.get_barrier_semaphore()
    others = [device(plane, peer) for peer in peers]
    others += [device(plane_at(step), chip) for step in range(1, planes)] + [partner]
    for other in others:
        pl.semaphore_signal(barrier, inc=1, device_id=(other,), device_id_type=MESH)
    pl.semaphore_wait(barrier, len(others))

    made = []

    def copy(slot, to, src=None, dst=None):
        at = len(made)
        made.append(
            pltpu.make_async_remote_copy(
                src_ref=whole_ref.at[slot] if src is None else src,
                dst_ref=whole_ref.at[slot] if dst is None else dst,
                send_sem=send.at[at], recv_sem=recv.at[at],
                device_id=(to,), device_id_type=MESH,
            )
        )
        made[-1].start()
        return made[-1]

    between = [copy(me, device(plane_at(step), chip), shard_ref) for step in range(1, planes)]
    within, final = [], []
    for age in (2, 1):
        final.append(copy(None, device(plane_at(age), chip), text_ref, texts_ref.at[age]))
    for step in range(planes + 1):
        if step < planes:
            held = plane_at(-step)
            slot = device(held, chip)
            if step > 0:
                between[step - 1].wait_recv()
            src = shard_ref if step == 0 else None
            within.append([copy(slot, device(plane, peer), src) for peer in peers])
            final.append(copy(slot, partner, src))
            if step == 0:
                whole_ref[me] = shard_ref[...]
                texts_ref[0] = text_ref[...]
        if step > 0:
            held = plane_at(1 - step)
            for at, source in enumerate(sources):
                within[step - 1][at].wait_recv()
                slot = device(held, source)
                if relayed and at == 0:
                    relay = copy(slot, device(plane, peers[1]))
                final.append(copy(slot, partner))
            if relayed:
                relay.wait_recv()
                final.append(copy(device(held, 3 - chip), partner))
    for one in final:
        one.wait_recv()
    for one in made:
        one.wait_send()


def gather(shard, text, count, group):
    planes, chips = count // group, group // 2
    copies = planes + 1 + planes * (2 * chips - 1)
    vmem = pl.BlockSpec(memory_space=pltpu.VMEM)
    return pl.pallas_call(
        functools.partial(gather_kernel, count, group),
        out_shape=[
            jax.ShapeDtypeStruct((count,) + shard.shape, shard.dtype),
            jax.ShapeDtypeStruct((3,) + text.shape, text.dtype),
        ],
        in_specs=[vmem] * 2,
        out_specs=[vmem] * 2,
        scratch_shapes=[pltpu.SemaphoreType.DMA((copies,)), pltpu.SemaphoreType.DMA((copies,))],
        compiler_params=pltpu.CompilerParams(
            collective_id=1, has_side_effects=True, vmem_limit_bytes=40 * 1024 * 1024
        ),
    )(shard, text)


def per_device(image_features, text_features, projections, labels):
    rows, width_in = image_features.shape
    count = lax.axis_size("dp")
    shifts = min(REACH, count // 2)
    whole, texts = gather(projections, text_features, count, shifts // 2)
    whole = whole.reshape(2 * width_in, -1)
    image_weight = whole[:width_in]
    text_weight = whole[width_in:]
    image_unit, image_norm = normalize(
        jnp.dot(image_features, image_weight, preferred_element_type=jnp.float32)
    )
    text_units, text_norms = normalize(
        jnp.dot(
            texts.reshape(3 * rows, width_in), text_weight, preferred_element_type=jnp.float32
        )
    )
    text_unit, text_norm = text_units[:rows], text_norms[:rows]
    image_acc, text_acc = pair_grads(
        image_unit.astype(jnp.bfloat16), text_units.astype(jnp.bfloat16), labels, count, shifts
    )
    image_draw = unproject(image_unit, image_norm, image_acc)
    text_draw = unproject(text_unit, text_norm, text_acc)
    image_grad = lax.dot_general(
        image_draw, image_weight, contract_last, preferred_element_type=jnp.float32
    )
    text_grad = lax.dot_general(
        text_draw, text_weight, contract_last, preferred_element_type=jnp.float32
    )
    return (image_grad, text_grad)


def solution(mesh):
    placed = (P("dp", None), P("dp", None), P("dp", None), P("dp"))
    return jax.shard_map(
        per_device,
        mesh=mesh,
        in_specs=placed,
        out_specs=(P("dp", None), P("dp", None)),
        check_vma=False,
    )
```
